256 devices in a mesh: groups: 4 (over y, x), rows: 64 (over z, core).
Axes of the slice: x: 2, y: 2, z: 32, core: 2. Of those that a mesh axis runs over, the one named last changes fastest.
The devices are a block of a 4x8x32 slice.
Arguments:
- queries: bfloat16 [4096, 8192], P(('groups', 'rows')), parts along dimension 0, may hold values from -6 to 6
- sketches: bfloat16 [131072, 8192], P(('groups', 'rows')), parts along dimension 0, may hold values from -16 to 16, as said below
- row_ids: int32 [131072], P(('groups', 'rows')), parts along dimension 0, may hold values from 0 to 32767, each once
Outputs:
- top_scores: float32 [4096, 128], P(('groups', 'rows')), parts along dimension 0
The draws below stay inside these ranges and needn't reach their ends.
There are 4 independent parts, one for each index of `groups`. The reference program is written for one: setup_inputs(seed, part) draws one part's arguments, and reference() takes and returns one part's arrays. A program takes and returns all parts, laid end to end along the dimension named above; each array names one. Nothing has to cross between parts.
Inputs may be any that keep to these rules, and one draw needn't show every extreme that they name: `sketches`: sketch entries are real-valued.
All inputs are finite; a program needn't handle non-finite values.
Results may differ from the reference program's by a relative error of at most 0.0003.
Values may be sent and summed in bfloat16 or wider, within the bound.
A program may use at most 128 MiB of HBM per device.

```python
import jax
import jax.numpy as jnp
from jax import lax

WIDTH = 8192
NQ = 1024
ROWS_DEV = 512
TOPK = 128
ROWS = 32768
RETIRED = 8192
N_ROWS = 64


def query_values(key):
    values = jax.random.normal(jax.random.fold_in(key, 21), (NQ, WIDTH), jnp.float32)
    return jnp.clip(values, -6.0, 6.0)


def draw_queries(key, part):
    return query_values(key).astype(jnp.bfloat16)


def draw_sketches(key, part):
    position = jnp.arange(ROWS).astype(jnp.float32)
    rising = 1.0 + 2.0 * position / jnp.float32(max(ROWS - 1, 1))
    row_scale = jnp.exp(jax.random.uniform(jax.random.fold_in(key, 11), (ROWS,), jnp.float32, 0.0, jnp.log(10.0)))
    base = jax.random.normal(jax.random.fold_in(key, 14), (ROWS, WIDTH), jnp.float32)
    values = base * (row_scale * rising)[:, None] / jnp.sqrt(jnp.float32(WIDTH))
    query_full = query_values(key)
    home_query = jax.random.permutation(jax.random.fold_in(key, 31), NQ).astype(jnp.int32)[:N_ROWS]
    device_of_row = jnp.arange(ROWS).astype(jnp.int32) // ROWS_DEV
    scattered = jax.random.randint(jax.random.fold_in(key, 33), (ROWS,), 0, NQ).astype(jnp.int32)
    home_pool = jax.random.randint(jax.random.fold_in(key, 34), (ROWS,), 0, 2).astype(jnp.int32) == 0
    target = jnp.where(home_pool, jnp.take(home_query, device_of_row, axis=0), scattered).astype(jnp.int32)
    direction = jnp.take(query_full, target, axis=0) / jnp.float32(WIDTH)
    amplitude = 120.0 * jnp.exp(jax.random.uniform(jax.random.fold_in(key, 32), (ROWS,), jnp.float32, jnp.log(1.5), jnp.log(3.0)))
    boosted = values + amplitude[:, None] * direction
    return jnp.clip(boosted, -16.0, 16.0).astype(jnp.bfloat16)


def setup_inputs(seed: int = 0, part: int = 0) -> dict:
    streams_of = jax.random.split(jax.random.key(seed), 4)
    part_splits = jax.random.split(jax.random.fold_in(streams_of[3], part), 4)
    queries = draw_queries(jax.random.fold_in(jax.random.fold_in(streams_of[3], part), 71), part)
    sketches = draw_sketches(jax.random.fold_in(jax.random.fold_in(streams_of[3], part), 71), part)
    row_ids = jax.random.permutation(part_splits[2], ROWS).astype(jnp.int32)
    return {"queries": queries, "sketches": sketches, "row_ids": row_ids}


def reference(queries, sketches, row_ids):
    scores = lax.dot_general(queries, sketches, (((1,), (1,)), ((), ())), preferred_element_type=jnp.float32)
    live = row_ids >= RETIRED
    square_sum = lax.optimization_barrier(jnp.sum(jnp.where(live[None, :], scores * scores, jnp.float32(0.0)), axis=1))
    inverse_scale = lax.rsqrt(square_sum / jnp.float32(ROWS - RETIRED) + jnp.float32(1e-06))
    masked = jnp.where(live[None, :], scores, jnp.float32(-1e+30))
    best = lax.top_k(masked, TOPK)[0]
    return best * inverse_scale[:, None]
```

```python
import functools

import jax
import jax.numpy as jnp
from jax import lax
from jax.experimental import pallas as pl
from jax.experimental.pallas import tpu as pltpu
from jax.sharding import PartitionSpec as P

TOPK = 128
LANES = 128
SUB = 8
CHUNKS = 8
DELAY = 3
DEAD = -1e30


def exchange(a, b):
    return jnp.maximum(a, b), jnp.minimum(a, b)


def sort_pairs(n):
    pairs = []

    def merge(lo, length, step):
        double = step * 2
        if double < length:
            merge(lo, length, double)
            merge(lo + step, length, double)
            for i in range(lo + step, lo + length - step, double):
                pairs.append((i, i + step))
        else:
            pairs.append((lo, lo + step))

    def sort(lo, length):
        if length > 1:
            half = length // 2
            sort(lo, half)
            sort(lo + half, half)
            merge(lo, length, 1)

    sort(0, n)
    return pairs


def descend(values, gap):
    values = list(values)
    while gap >= 1:
        for i in range(len(values)):
            if i % (2 * gap) < gap:
                values[i], values[i + gap] = exchange(values[i], values[i + gap])
        gap //= 2
    return values


class Rows:
    def __init__(self, ref, base=0):
        self.ref, self.base = ref, base

    def at(self, i):
        start = (self.base + i) * SUB
        if not isinstance(start, int):
            start = pl.multiple_of(start, SUB)
        return pl.ds(start, SUB)

    def load(self, i):
        return self.ref[self.at(i), :]

    def store(self, i, value):
        self.ref[self.at(i), :] = value


def finish(rows, count):
    for block in range(0, count, 16):
        values = descend([rows.load(block + i) for i in range(16)], 8)
        for i in range(16):
            rows.store(block + i, values[i])


def join(rows, size):
    half = size // 2
    firsts = range(0, half, 16)
    for i in range(16):
        index = [i + k for k in firsts] + [size - 1 - i - k for k in reversed(firsts)]
        low = len(firsts)
        values = [rows.load(k) for k in index]
        for k in range(low):
            values[k], values[2 * low - 1 - k] = exchange(values[k], values[2 * low - 1 - k])
        values = descend(values[:low], low // 2) + descend(values[low:], low // 2)
        for k, value in zip(index, values):
            rows.store(k, value)
    finish(rows, size)


def prune(left, right, out, keep, view=lambda value: value):
    for i in range(16):
        index = list(range(i, keep, 16))
        values = [jnp.maximum(left.load(k), view(right.load(keep - 1 - k))) for k in index]
        values = descend(values, len(index) // 2)
        for k, value in zip(index, values):
            out.store(k, value)
    finish(out, keep)


def sort_rows(ref, count, keep):
    network = sort_pairs(16)

    @pl.loop(0, count // 16)
    def _(block):
        rows = Rows(ref, block * 16)
        values = [rows.load(i) for i in range(16)]
        for a, b in network:
            values[a], values[b] = exchange(values[a], values[b])
        for i in range(16):
            rows.store(i, values[i])

    @pl.loop(0, count // 32)
    def _(block):
        rows = Rows(ref, block * 32)
        values = [rows.load(i) for i in range(32)]
        for i in range(16):
            values[i], values[31 - i] = exchange(values[i], values[31 - i])
        values = descend(values[:16], 8) + descend(values[16:], 8)
        for i in range(32):
            rows.store(i, values[i])

    size = 64
    while size <= keep:

        @pl.loop(0, count // size)
        def _(block, size=size):
            join(Rows(ref, block * size), size)

        size *= 2

    runs = count // keep
    gap = 1
    while gap < runs:

        @pl.loop(0, runs // (2 * gap))
        def _(pair, gap=gap):
            left = Rows(ref, pair * (2 * gap * keep))
            right = Rows(ref, pair * (2 * gap * keep) + gap * keep)
            prune(left, right, left, keep)

        gap *= 2


def kernel(
    chips, retired, live_count,
    queries, sketches, row_ids, out,
    gathered, rows, live, total, scores, square, lists, square_in, other, sent, received, square_received,
    load_sem, link_send, link_recv, die_send, die_recv, pair_send, pair_recv, list_send, list_recv, sum_send, sum_recv,
):
    count, width = rows.shape
    own = queries.shape[0]
    columns = width // CHUNKS
    per_batch = LANES // (2 * own)
    pieces = per_batch * CHUNKS
    depth = width // pieces
    batches = chips // per_batch
    me = lax.axis_index("rows")
    chip, core = me // 2, me % 2
    step = 1 - 2 * core
    following = {"rows": ((chip + chips + step) % chips) * 2 + core}
    previous = {"rows": ((chip + chips - step) % chips) * 2 + core}
    sibling = {"rows": chip * 2 + (1 - core)}
    mesh_id = pl.DeviceIdType.MESH

    def place(distance, stream):
        return pl.ds(pl.multiple_of((distance * 2 + stream) * own, own), own)

    def part(j):
        return pl.ds(pl.multiple_of(j * columns, LANES), columns)

    def over_link(distance, j):
        return pltpu.make_async_remote_copy(
            gathered.at[place(distance, core), part(j)],
            gathered.at[place(distance + 1, core), part(j)],
            link_send.at[distance % 2, j], link_recv.at[distance + 1, j],
            device_id=following, device_id_type=mesh_id,
        )

    def over_die(distance, j):
        return pltpu.make_async_remote_copy(
            gathered.at[place(distance, core), part(j)],
            gathered.at[place(distance, core), part(j)],
            die_send.at[distance % 2, j], die_recv.at[distance, j],
            device_id=sibling, device_id_type=mesh_id,
        )

    load_queries = pltpu.make_async_copy(queries, gathered.at[place(0, core), :], load_sem.at[0])
    load_queries.start()
    load_rows = pltpu.make_async_copy(sketches, rows, load_sem.at[1])
    load_rows.start()
    barrier = pltpu.get_barrier_semaphore()
    for device in (following, previous, sibling):
        pl.semaphore_signal(barrier, inc=1, device_id=device, device_id_type=mesh_id)

    for block in range(count // LANES):
        ids = row_ids[pl.ds(block, 1), :]
        flags = jnp.where(ids >= retired, jnp.float32(1.0), jnp.float32(0.0))
        live[pl.ds(block * LANES, LANES), :] = jnp.broadcast_to(flags, (LANES, LANES)).T
    load_queries.wait()
    pl.semaphore_wait(barrier, 3)

    def compute(piece):
        batch, k = piece // pieces, piece % pieces

        @pl.when(k == 0)
        def _():
            @pl.loop(0, pieces)
            def _(index):
                over_die(batch * per_batch + index // CHUNKS, index % CHUNKS).wait_recv()

            total[...] = jnp.zeros_like(total)

        cut = pl.ds(pl.multiple_of(k * depth, LANES), depth)
        total[...] += lax.dot_general(
            rows[:, cut],
            gathered[pl.ds(pl.multiple_of(batch * LANES, LANES), LANES), cut],
            (((1,), (1,)), ((), ())),
            preferred_element_type=jnp.float32,
        )

        @pl.when(k == pieces - 1)
        def _():
            kept = live[...] > 0.5
            value = total[...]
            squares = jnp.where(kept, value * value, jnp.float32(0.0))
            square[batch] = jnp.sum(squares, axis=0, keepdims=True)
            scores[pl.ds(batch, count, stride=SUB), :] = jnp.where(kept, value, jnp.float32(DEAD))

    first = per_batch * CHUNKS + DELAY

    @pl.loop(0, chips * CHUNKS)
    def _(slot):
        distance, j = slot // CHUNKS, slot % CHUNKS

        @pl.when(distance > 0)
        def _():
            over_link(distance - 1, j).wait_recv()

        @pl.when(distance < chips - 1)
        def _():
            @pl.when(distance >= 2)
            def _():
                over_link(distance - 2, j).wait_send()

            over_link(distance, j).start()

        @pl.when(distance >= 2)
        def _():
            over_die(distance - 2, j).wait_send()

        over_die(distance, j).start()

        @pl.when(slot == first)
        def _():
            load_rows.wait()

        @pl.when(slot >= first)
        def _():
            compute(slot - first)

    @pl.loop(chips * CHUNKS - first, batches * pieces)
    def _(piece):
        compute(piece)

    @pl.loop(0, 2 * CHUNKS)
    def _(index):
        over_link(chips - 3 + index // CHUNKS, index % CHUNKS).wait_send()
        over_die(chips - 2 + index // CHUNKS, index % CHUNKS).wait_send()

    sort_rows(scores, count, TOPK)

    @pl.loop(0, TOPK)
    def _(i):
        at = pl.ds(pl.multiple_of(i * SUB, SUB), SUB)
        lists[at, :] = scores[at, :]

    to_sibling = pltpu.make_async_remote_copy(
        lists, other, pair_send.at[0], pair_recv.at[0], device_id=sibling, device_id_type=mesh_id
    )
    to_sibling.start()
    sums_to_sibling = pltpu.make_async_remote_copy(
        square, square_in, pair_send.at[1], pair_recv.at[1], device_id=sibling, device_id_type=mesh_id
    )
    sums_to_sibling.start()
    to_sibling.wait()
    sums_to_sibling.wait()
    square_in[...] = square_in[...] + square[...]
    prune(Rows(lists), Rows(other), Rows(scores), TOPK)

    for batch in range(batches):
        sent[pl.ds(batch * LANES, LANES), :] = scores[pl.ds(batch, TOPK, stride=SUB), :].T

    def owner(distance):
        return {"rows": ((chip + chips - step * distance) % chips) * 2 + core}

    def list_out(distance):
        return pltpu.make_async_remote_copy(
            sent.at[place(distance, core), :],
            received.at[pl.ds(pl.multiple_of(distance * own, own), own), :],
            list_send.at[distance], list_recv.at[distance],
            device_id=owner(distance), device_id_type=mesh_id,
        )

    def sum_out(distance):
        return pltpu.make_async_remote_copy(
            square_in.at[distance // per_batch],
            square_received.at[distance],
            sum_send.at[distance], sum_recv.at[distance],
            device_id=owner(distance), device_id_type=mesh_id,
        )

    half = chips // 2

    @pl.loop(0, chips - 1)
    def _(index):
        near = half - (index + 1) // 2
        distance = jnp.where(index % 2 == 0, near, chips - near)
        list_out(distance).start()
        sum_out(distance).start()

    received[pl.ds(0, own), :] = sent[place(0, core), :]
    square_received[0] = square_in[0]

    @pl.loop(1, chips)
    def _(distance):
        list_out(distance).wait()
        sum_out(distance).wait()

    row = jnp.zeros((1, LANES), jnp.float32)
    for inside in range(per_batch):
        term = square_received[inside]
        for batch in range(1, batches):
            term = term + square_received[batch * per_batch + inside]
        shift = inside * 2 * own
        row = row + (pltpu.roll(term, LANES - shift, 1) if shift else term)
    row = jnp.where(core == 0, row, pltpu.roll(row, LANES - own, 1))
    squares = jnp.broadcast_to(row, (LANES, LANES)).T[:own, :]
    inverse = lax.rsqrt(squares / jnp.float32(live_count) + jnp.float32(1e-6))

    held = chips * own // LANES
    for block in range(held):
        scores[pl.ds(block, TOPK, stride=SUB), :] = received[pl.ds(block * LANES, LANES), :].T
    source, target = scores, lists
    views = []
    gap = held // 2
    while gap >= 1:
        views.append((0, SUB - gap))
        gap //= 2
    gap = LANES // 2
    while gap >= own:
        views.append((1, LANES - gap))
        gap //= 2
    for axis, shift in views:
        prune(
            Rows(source), Rows(source), Rows(target), TOPK,
            lambda value, axis=axis, shift=shift: pltpu.roll(value, shift, axis),
        )
        source, target = target, (scores if target is lists else lists)
    best = source[pl.ds(0, TOPK, stride=SUB), :].T[:own, :]
    out[...] = best * inverse


def shards(queries, sketches, row_ids):
    devices = lax.axis_size("rows")
    chips = devices // 2
    count, width = sketches.shape
    own = queries.shape[0]
    total_rows = count * devices
    retired = total_rows // 4
    per_batch = LANES // (2 * own)
    batches = chips // per_batch
    f32 = jnp.float32
    dma = pltpu.SemaphoreType.DMA
    return pl.pallas_call(
        functools.partial(kernel, chips, retired, total_rows - retired),
        out_shape=jax.ShapeDtypeStruct((own, TOPK), f32),
        in_specs=[
            pl.BlockSpec(memory_space=pl.ANY),
            pl.BlockSpec(memory_space=pl.ANY),
            pl.BlockSpec(memory_space=pltpu.VMEM),
        ],
        out_specs=pl.BlockSpec(memory_space=pltpu.VMEM),
        scratch_shapes=[
            pltpu.VMEM((devices * own, width), jnp.bfloat16),
            pltpu.VMEM((count, width), jnp.bfloat16),
            pltpu.VMEM((count, LANES), f32),
            pltpu.VMEM((count, LANES), f32),
            pltpu.VMEM((count * SUB, LANES), f32),
            pltpu.VMEM((batches, 1, LANES), f32),
            pltpu.VMEM((TOPK * SUB, LANES), f32),
            pltpu.VMEM((batches, 1, LANES), f32),
            pltpu.VMEM((TOPK * SUB, LANES), f32),
            pltpu.VMEM((devices * own, TOPK), f32),
            pltpu.VMEM((chips * own, TOPK), f32),
            pltpu.VMEM((chips, 1, LANES), f32),
            dma((2,)),
            dma((2, CHUNKS)), dma((chips, CHUNKS)),
            dma((2, CHUNKS)), dma((chips, CHUNKS)),
            dma((2,)), dma((2,)),
            dma((chips,)), dma((chips,)), dma((chips,)), dma((chips,)),
        ],
        compiler_params=pltpu.CompilerParams(
            collective_id=0, has_side_effects=True, vmem_limit_bytes=60 * 1024 * 1024
        ),
        name="attribute",
    )(queries, sketches, row_ids.reshape(count // LANES, LANES))


def solution(mesh):
    return jax.shard_map(
        shards,
        mesh=mesh,
        in_specs=(P(("groups", "rows"), None), P(("groups", "rows"), None), P(("groups", "rows"))),
        out_specs=P(("groups", "rows"), None),
        check_vma=False,
    )
```
